32 devices in a mesh: dp: 16 (over z, x, core), mp: 2 (over y).
Axes of the slice: x: 2, y: 2, z: 4, core: 2. Of those that a mesh axis runs over, the one named last changes fastest.
Arguments:
- grads: bfloat16 [16, 24, 512, 512], P('dp', None, 'mp'), may hold values from -0.0625 to 0.0625
- owners: int32 [24, 1], replicated, may hold values from 0 to 15; in each aligned block of 24 rows (0 to 23, 24 to 47, ...) at most 4 rows name the same one
- left_stat: float32 [16, 4, 512, 512], P('dp', None, 'mp'), as said below
- right_stat: float32 [16, 4, 512, 512], P('dp', None, 'mp'), as said below
- first_moment: float32 [16, 4, 512, 512], P('dp', None, 'mp'), may hold values from -0.3 to 0.3
- second_moment: float32 [16, 4, 512, 512], P('dp', None, 'mp'), may hold values from 0.0001 to 0.01
Outputs:
- direction: bfloat16 [24, 512, 512], P(None, 'mp')
- left_out: float32 [16, 4, 512, 512], P('dp', None, 'mp')
- right_out: float32 [16, 4, 512, 512], P('dp', None, 'mp')
- first_out: float32 [16, 4, 512, 512], P('dp', None, 'mp')
- second_out: float32 [16, 4, 512, 512], P('dp', None, 'mp')
The draws below stay inside these ranges and needn't reach their ends.
Inputs may be any that keep to these rules, and one draw needn't show every extreme that they name: `owners`: no owner holds more than 4 blocks, some owner holds exactly 4, and every owner holds at least one. `left_stat`: each slot's matrix is symmetric positive definite. `right_stat`: each slot's matrix is symmetric positive definite.
All inputs are finite; a program needn't handle non-finite values.
Results may differ from the reference program's by a relative error of at most 0.025.
Values may be sent and summed in bfloat16 or wider, within the bound.
No kernel may reach another device: no remote copies, remote signals or barrier semaphores. Data moves between devices by JAX's collectives and lax.ppermute only.
A program may use at most 128 MiB of HBM per device.

```python
import math
import jax
import jax.numpy as jnp
import numpy as np
from jax import lax

B = 512
ITERS = 6
MOST = 4
NB = 24
N_DP = 16


def definite_draw(key):

    def one_owner(owner_key):
        normals = jax.random.normal(owner_key, (MOST, B, 2 * B), jnp.float32)
        matrices = jnp.einsum('sik,sjk->sij', normals, normals, precision=lax.Precision.HIGHEST) / (2.0 * B)
        return matrices
    owner_keys = jax.random.split(key, N_DP)
    return lax.map(one_owner, owner_keys)


def draw_left_stat(key, part):
    return definite_draw(jax.random.fold_in(key, 11))


def draw_right_stat(key, part):
    return definite_draw(jax.random.fold_in(key, 23))


def shard_levels(stream_key, shape, shards, smallest, high):
    loudness, own = 1.0, jax.random.fold_in(stream_key, 6)
    for dim, parts in shards:
        draws = jnp.exp(jax.random.uniform(jax.random.fold_in(own, dim), (parts,), jnp.float32, smallest / len(shards), high / len(shards)))
        loudness = loudness * jnp.repeat(draws, shape[dim] // parts).reshape([-1 if axis == dim else 1 for axis in range(len(shape))])
    return loudness


def deal_out(rng, own, number, rows, number_of, top, limit, skew):
    sequence = jax.random.permutation(rng, number_of)
    heavy_load, ordinary = portions_of(number_of, rows * top, limit, skew, True), portions_of(number_of, rows * top, limit, skew, False)
    places = jnp.arange(number_of)

    def named(tallies, offset_by):
        used = int((tallies > 0).sum())
        fixed = max(1, used // 4)
        passed = fixed + (places - fixed + offset_by * (used - fixed)) % max(1, number_of - fixed)
        return jnp.zeros((number_of,), jnp.int32).at[sequence[jnp.where(places < fixed, places, passed)]].set(jnp.asarray(tallies, jnp.int32))

    tallies = jnp.where(number % 4 == 0, named(heavy_load, number // 4), named(ordinary, number - number // 4 - 1))
    mixed = jax.random.permutation(jax.random.fold_in(own, 3), number_of)
    giver, taker = mixed[0:number_of // 2 * 2:2], mixed[1:number_of // 2 * 2:2]
    room = jnp.minimum(tallies[giver] - 1, limit - tallies[taker]) // 2
    room = jnp.where((giver == sequence[0]) | (taker == sequence[0]) | (tallies[taker] == 0), 0, jnp.maximum(room, 0))
    passed = jax.random.randint(jax.random.fold_in(own, 4), (number_of // 2,), 0, 1 << 20) % (room + 1)
    tallies = tallies.at[giver].add(-passed).at[taker].add(passed)
    labels = jnp.searchsorted(jnp.cumsum(tallies), jnp.arange(rows * top), side="right").astype(jnp.int32)
    table = labels.reshape(top, rows).T
    table = table[jax.random.permutation(jax.random.fold_in(own, 1), rows)]
    offset_by = jax.random.randint(jax.random.fold_in(own, 2), (rows, 1), 0, top)
    return jnp.take_along_axis(table, (jnp.arange(top)[None, :] + offset_by) % top, axis=1)


def portions_of(count, total, reach, slope, full):
    weights = [(1 << 20) // math.isqrt(grade ** slope) + 1 for grade in range(1, count + 1)]
    largest = reach if full else min(reach, max(-(-total // count), total * weights[0] // sum(weights)))
    least = 1 if total - largest >= count - 1 else 0
    holding, surplus = [largest] + [least] * (count - 1), total - largest - least * (count - 1)
    while surplus > 0:
        free = [i for i in range(1, count) if holding[i] < largest] or [i for i in range(1, count) if holding[i] < reach]
        whole, left = sum([weights[i] for i in free]), surplus
        for i in free:
            extra = min(reach - holding[i], max(1, left * weights[i] // whole), surplus)
            holding[i] = holding[i] + extra
            surplus = surplus - extra
    return np.array(holding)


def normal_values(own_key, extent, width, bound, cuts=(), kind=jnp.bfloat16):
    factor_of = shard_levels(own_key, extent, cuts, -0.22, 0.18) if cuts else 1.0
    drawn = jax.random.normal(own_key, extent, jnp.float32) * width * factor_of
    return jnp.minimum(jnp.maximum(drawn, -bound), bound).astype(kind)


def setup_inputs(seed: int = 0) -> dict:
    key_of = jax.random.split(jax.random.key(seed), 7)
    grads = normal_values(key_of[0], (N_DP, NB, B, B), (N_DP * B) ** -0.5, 0.0625, ((0, 16), (2, 2)))
    owners_keys = jax.random.split(jax.random.fold_in(key_of[1], 1), NB // NB)
    owners_turns = jax.random.permutation(jax.random.fold_in(key_of[1], 3), NB // NB)
    owners = jax.vmap(lambda own, number: deal_out(jax.random.fold_in(key_of[1], 2), own, number, NB, N_DP, 1, MOST, 2))(owners_keys, owners_turns).reshape((NB, 1))
    left_stat = draw_left_stat(jax.random.fold_in(key_of[6], 71), 0)
    right_stat = draw_right_stat(jax.random.fold_in(key_of[6], 71), 0)
    first_moment = normal_values(key_of[4], (N_DP, MOST, B, B), 0.05, 0.3, ((0, 16), (2, 2)), jnp.float32)
    second_moment = jnp.clip(jnp.exp(math.log(0.01) - 4.6051702 * jax.random.uniform(key_of[5], (N_DP, MOST, B, B), jnp.float32) ** shard_levels(key_of[5], (N_DP, MOST, B, B), ((0, 16), (2, 2)), -0.2, 0.2)), 0.0001, 0.01)
    return {"grads": grads, "owners": owners, "left_stat": left_stat, "right_stat": right_stat, "first_moment": first_moment, "second_moment": second_moment}


HIGHEST_PRECISION = lax.Precision.HIGHEST

def matmul(left, right):
    return jnp.matmul(left.astype(jnp.float32), right.astype(jnp.float32), precision=HIGHEST_PRECISION)

def inverse_root(matrix):
    order_size = matrix.shape[-1]
    identity = jnp.eye(order_size, dtype=jnp.float32)
    frobenius = jnp.sqrt(jnp.sum(matrix * matrix))
    scaling = 5.0 / (2.0 * frobenius)
    current = (scaling * matrix).astype(jnp.bfloat16)
    root_now = (identity * scaling ** 0.25).astype(jnp.bfloat16)
    for sweep in range(ITERS):
        factor_now = ((5.0 * identity - current.astype(jnp.float32)) / 4.0).astype(jnp.bfloat16)
        root_now = matmul(root_now, factor_now).astype(jnp.bfloat16)
        power_now = matmul(factor_now, factor_now).astype(jnp.bfloat16)
        power_now = matmul(power_now, factor_now).astype(jnp.bfloat16)
        power_now = matmul(power_now, factor_now).astype(jnp.bfloat16)
        current = matmul(power_now, current).astype(jnp.bfloat16)
    return root_now

def block_step(items):
    summed_grad, left_old, right_old, first_old, second_old = items
    rounded = summed_grad.astype(jnp.bfloat16)
    left_new = 0.9 * left_old + 0.1 * matmul(rounded, rounded.T)
    right_new = 0.9 * right_old + 0.1 * matmul(rounded.T, rounded)
    left_root = inverse_root(left_new)
    right_root = inverse_root(right_new)
    left_half = matmul(left_root, rounded).astype(jnp.bfloat16)
    shampoo = matmul(left_half, right_root)
    first_new = 0.9 * first_old + 0.1 * summed_grad
    second_new = 0.95 * second_old + 0.05 * summed_grad * summed_grad
    adam_step = first_new / (jnp.sqrt(second_new) + 1e-08)
    adam_rows = jnp.sqrt(lax.optimization_barrier(jnp.sum(adam_step * adam_step, axis=1, keepdims=True)))
    shampoo_rows = jnp.sqrt(lax.optimization_barrier(jnp.sum(shampoo * shampoo, axis=1, keepdims=True))) + 1e-06
    direction = (shampoo * (adam_rows / shampoo_rows)).astype(jnp.bfloat16)
    return (direction, left_new, right_new, first_new, second_new)

def reference(grads, owners, left_stat, right_stat, first_moment, second_moment):
    owner_of = owners[:, 0].astype(jnp.int32)
    same_owner = (owner_of[:, None] == owner_of[None, :]).astype(jnp.int32)
    positions = jnp.arange(NB, dtype=jnp.int32)
    earlier = (positions[None, :] < positions[:, None]).astype(jnp.int32)
    slot_of = lax.optimization_barrier(jnp.sum(same_owner * earlier, axis=1)).astype(jnp.int32)
    summed = lax.optimization_barrier(jnp.sum(grads.astype(jnp.float32), axis=0))
    items = (summed, left_stat[owner_of, slot_of], right_stat[owner_of, slot_of], first_moment[owner_of, slot_of], second_moment[owner_of, slot_of])
    direction, left_new, right_new, first_new, second_new = lax.map(block_step, items)
    left_out = left_stat.at[owner_of, slot_of].set(left_new)
    right_out = right_stat.at[owner_of, slot_of].set(right_new)
    first_out = first_moment.at[owner_of, slot_of].set(first_new)
    second_out = second_moment.at[owner_of, slot_of].set(second_new)
    return (direction, left_out, right_out, first_out, second_out)
```

```python
import functools

import jax
import jax.numpy as jnp
from jax import lax
from jax.experimental import pallas as pl
from jax.experimental.pallas import tpu as pltpu
from jax.sharding import PartitionSpec as P

ITERS = 6
OUTER = 4
BF = jnp.bfloat16
F32 = jnp.float32
SMEM = pl.BlockSpec(memory_space=pltpu.SMEM)
VMEM = pl.BlockSpec(memory_space=pltpu.VMEM)
ANY = pl.BlockSpec(memory_space=pl.ANY)


def params(mib=48):
    return pltpu.CompilerParams(vmem_limit_bytes=mib << 20)


def cost(us):
    return pl.CostEstimate(flops=int(us * 9e8), bytes_accessed=int(us * 1e6), transcendentals=0)


def shape(*dims, dtype=BF):
    return jax.ShapeDtypeStruct(dims, dtype)


def product(left, right):
    return jnp.dot(left, right, preferred_element_type=F32)


def transposed(value):
    return value.astype(F32).T.astype(BF)


class Plan:
    def __init__(self, n, slots, blocks):
        self.n, self.slots, self.blocks = n, slots, blocks
        self.mid = n // (2 * OUTER)
        self.half = n // 2
        at = 0
        for name, size in (
            ("send", self.half),
            ("keep", self.half),
            ("extra", self.half),
            ("code", self.half),
            ("final", n),
            ("xfinal", self.half),
            ("xindex", self.half),
            ("mine", slots),
            ("place", slots),
            ("held", slots),
            ("core", 1),
            ("row", 1),
        ):
            setattr(self, name, at)
            at += size
        self.size = at


def plan_kernel(plan, pos_ref, own_ref, out_ref, count, first, xblock, xowner, xslot, seen):
    p, y = pos_ref[0], pos_ref[1]
    c = lax.rem(p, 2)
    q = lax.div(p, 2)
    mm = lax.rem(q, plan.mid)
    o = lax.div(q, plan.mid)
    for i in range(plan.n):
        count[i] = 0
        first[i] = 0
    for i in range(plan.half):
        xblock[i] = 0
        xowner[i] = 0
        xslot[i] = 1
    seen[0] = 0

    def visit(b, carry):
        w = own_ref[b]
        s = count[w]
        count[w] = s + 1

        @pl.when(s == 0)
        def _():
            first[w] = b

        @pl.when(s > 0)
        def _():
            e = seen[0]
            xblock[e] = b
            xowner[e] = w
            xslot[e] = s
            seen[0] = e + 1

        return carry

    lax.fori_loop(0, plan.blocks, visit, 0)
    for jm in range(plan.mid):
        for jo in range(OUTER):
            j = jm * OUTER + jo
            to = lax.rem(o + jo, OUTER) * plan.mid + lax.rem(mm + jm, plan.mid)
            out_ref[plan.send + j] = first[to * 2 + 1 - c]
            out_ref[plan.keep + j] = first[to * 2 + c]
            out_ref[plan.extra + j] = xblock[to]
            w, s = xowner[to], xslot[to] - 1
            others = plan.slots - 1
            out_ref[plan.code + j] = jnp.where(
                w == p, s, jnp.where(w == p + 1 - 2 * c, others + s, 2 * others)
            )
            source = lax.rem(o + OUTER - jo, OUTER) * plan.mid + lax.rem(mm + plan.mid - jm, plan.mid)
            out_ref[plan.final + j] = first[source * 2 + c]
            out_ref[plan.final + plan.half + j] = first[source * 2 + 1 - c]
            out_ref[plan.xfinal + j] = xblock[source]
            out_ref[plan.xindex + j] = source
    for s in range(plan.slots):
        out_ref[plan.mine + s] = 0
        out_ref[plan.place + s] = 0
        out_ref[plan.held + s] = 1 if s == 0 else 0

    def look(e, carry):
        @pl.when(xowner[e] == p)
        def _():
            s = xslot[e]
            out_ref[plan.mine + s] = e
            eo, em = lax.div(e, plan.mid), lax.rem(e, plan.mid)
            out_ref[plan.place + s] = (
                lax.rem(mm + plan.mid - em, plan.mid) * OUTER + lax.rem(o + OUTER - eo, OUTER)
            )
            out_ref[plan.held + s] = 1

        return carry

    lax.fori_loop(0, plan.half, look, 0)
    out_ref[plan.core] = c
    out_ref[plan.row] = y


def make_plan(plan, pos, owners):
    ints = lambda k: pltpu.SMEM((k,), jnp.int32)
    return pl.pallas_call(
        functools.partial(plan_kernel, plan),
        out_shape=shape(plan.size, dtype=jnp.int32),
        in_specs=[SMEM, SMEM],
        out_specs=SMEM,
        scratch_shapes=[ints(plan.n), ints(plan.n)] + [ints(plan.half)] * 3 + [ints(1)],
        cost_estimate=cost(2),
    )(pos, owners)


def pick_kernel(plan, plan_ref, grads_ref, first_out, extra_out, sems):
    c = plan_ref[plan.core]
    half_rows = extra_out.shape[1]
    copies = []
    for j in range(plan.half):
        copies.append(
            pltpu.make_async_copy(
                grads_ref.at[0, plan_ref[plan.send + j]], first_out.at[j], sems.at[j]
            )
        )
    for j in range(plan.half):
        rows = pl.ds(pl.multiple_of((1 - c) * half_rows, half_rows), half_rows)
        copies.append(
            pltpu.make_async_copy(
                grads_ref.at[0, plan_ref[plan.extra + j], rows],
                extra_out.at[j],
                sems.at[plan.half + j],
            )
        )
    for copy in copies:
        copy.start()
    for copy in copies:
        copy.wait()


def pick(plan, plan_array, grads):
    rows, columns = grads.shape[2:]
    return pl.pallas_call(
        functools.partial(pick_kernel, plan),
        out_shape=(shape(plan.half, rows, columns), shape(plan.half, rows // 2, columns)),
        in_specs=[SMEM, ANY],
        out_specs=(VMEM, VMEM),
        scratch_shapes=[pltpu.SemaphoreType.DMA((plan.n,))],
        compiler_params=params(),
        cost_estimate=cost(4),
    )(plan_array, grads)


def add_first_kernel(plan, plan_ref, grads_ref, got_ref, *rest):
    outs, (own, sems) = rest[:-2], rest[-2:]
    copies = [
        pltpu.make_async_copy(grads_ref.at[0, plan_ref[plan.keep + j]], own.at[j], sems.at[j])
        for j in range(plan.half)
    ]
    for copy in copies:
        copy.start()
    for j, copy in enumerate(copies):
        copy.wait()
        outs[j][...] = (own[j].astype(F32) + got_ref[j].astype(F32)).astype(BF)


def add_first(plan, plan_array, grads, got):
    rows, columns = grads.shape[2:]
    return pl.pallas_call(
        functools.partial(add_first_kernel, plan),
        out_shape=[shape(rows, columns)] * plan.half,
        in_specs=[SMEM, ANY, VMEM],
        out_specs=[VMEM] * plan.half,
        scratch_shapes=[
            pltpu.VMEM((plan.half, rows, columns), BF),
            pltpu.SemaphoreType.DMA((plan.half,)),
        ],
        compiler_params=params(),
        cost_estimate=cost(4),
    )(plan_array, grads, got)


def add_extra_kernel(plan, plan_ref, grads_ref, got_ref, left_ref, right_ref, mate_ref, *rest):
    outs, (own, stats, stack, sems) = rest[:-4], rest[-4:]
    c = plan_ref[plan.core]
    half_rows = got_ref.shape[1]
    others = plan.slots - 1
    rows = pl.ds(pl.multiple_of(c * half_rows, half_rows), half_rows)
    grad_copies = [
        pltpu.make_async_copy(
            grads_ref.at[0, plan_ref[plan.extra + j], rows], own.at[j], sems.at[j]
        )
        for j in range(plan.half)
    ]
    stat_copies = [
        pltpu.make_async_copy(
            ref.at[0, 1 + s, rows], stats.at[s, side], sems.at[plan.half + s * 2 + side]
        )
        for s in range(others)
        for side, ref in enumerate((left_ref, right_ref))
    ]
    for copy in stat_copies + grad_copies:
        copy.start()
    for copy in stat_copies:
        copy.wait()
    for s in range(others):
        for side in range(2):
            stack[s, side] = stats[s, side].astype(BF)
            stack[others + s, side] = mate_ref[side, s]
    for side in range(2):
        stack[2 * others, side] = jnp.zeros(stack.shape[2:], BF)
    for j, copy in enumerate(grad_copies):
        copy.wait()
        code = plan_ref[plan.code + j]
        outs[j][0:half_rows] = (own[j].astype(F32) + got_ref[j].astype(F32)).astype(BF)
        outs[j][half_rows : 2 * half_rows] = stack[code, 0]
        outs[j][2 * half_rows : 3 * half_rows] = stack[code, 1]


def add_extra(plan, plan_array, grads, got, left, right, mate):
    half_rows, columns = got.shape[1:]
    others = plan.slots - 1
    return pl.pallas_call(
        functools.partial(add_extra_kernel, plan),
        out_shape=[shape(3 * half_rows, columns)] * plan.half,
        in_specs=[SMEM, ANY, VMEM, ANY, ANY, VMEM],
        out_specs=[VMEM] * plan.half,
        scratch_shapes=[
            pltpu.VMEM((plan.half, half_rows, columns), BF),
            pltpu.VMEM((others, 2, half_rows, columns), F32),
            pltpu.VMEM((2 * others + 1, 2, half_rows, columns), BF),
            pltpu.SemaphoreType.DMA((plan.half + 2 * others,)),
        ],
        compiler_params=params(),
        cost_estimate=cost(5),
    )(plan_array, grads, got, left, right, mate)


class Moves:
    def __init__(self, n, m):
        self.n, self.m, self.mid = n, m, n // (2 * OUTER)

    def _dp(self, value, to):
        return lax.ppermute(value, "dp", [(i, to(i)) for i in range(self.n)])

    def core(self, value):
        return self._dp(value, lambda i: i ^ 1)

    def middle(self, value, shift):
        mid = self.mid
        return self._dp(
            value,
            lambda i: (i // (2 * mid) * mid + (i // 2 + shift) % mid) * 2 + i % 2
            if mid > 1
            else i,
        )

    def outer(self, value, shift):
        step = 2 * self.mid
        return self._dp(value, lambda i: (i + shift * step) % self.n)

    def rows(self, value):
        m = self.m
        return [value] + [
            lax.ppermute(value, "mp", [(i, (i + s) % m) for i in range(m)]) for s in range(1, m)
        ]


def total_of(terms):
    total = terms[0].astype(F32)
    for term in terms[1:]:
        total = total + term.astype(F32)
    return total.astype(BF)


def scatter(moves, pieces):
    sums = [None] * OUTER
    for jo in (2, 1, 3, 0):
        terms = [pieces[jo]]
        for jm in range(1, moves.mid):
            terms.append(moves.middle(pieces[jm * OUTER + jo], jm))
        sums[jo] = total_of(terms)
    return total_of([sums[0]] + [moves.outer(sums[jo], jo) for jo in (2, 1, 3)])


def gather(moves, piece):
    near = [piece] + [moves.outer(piece, jo) for jo in range(1, OUTER)]
    own = [jnp.stack(near)]
    for jm in range(1, moves.mid):
        own.append(jnp.stack([moves.middle(value, jm) for value in near]))
    return own, [moves.core(value) for value in own]


def root_rows(off, rows, g_s, gt_s, stats, a_s, m_s, f_s, u_s, w_s, x_s):
    order = g_s.shape[0]
    diagonal = lax.broadcasted_iota(jnp.int32, (order, order), 0) == lax.broadcasted_iota(
        jnp.int32, (order, order), 1
    )
    gt_s[...] = transposed(g_s[...])

    def factor(side):
        five = jnp.where(diagonal, 5.0, 0.0)
        return ((five - m_s[side].astype(F32)) * 0.25).astype(BF)

    for side, (left, right) in enumerate(((g_s, gt_s), (gt_s, g_s))):
        a_s[side] = 0.9 * stats[side].astype(F32) + 0.1 * product(left[...], right[...])
        a = a_s[side]
        square = jnp.sum(jnp.sum(a * a, axis=1, keepdims=True), axis=0, keepdims=True)
        z = 5.0 / (2.0 * jnp.sqrt(square))
        m_s[side] = (z * a).astype(BF)
        f = factor(side)
        f_s[side] = f
        start = jnp.sqrt(jnp.sqrt(z)).astype(BF).astype(F32)
        x_s[side] = (start * f.astype(F32)).astype(BF)

    def sweep(k, carry):
        block = order // 2
        for side in range(2):
            u_s[side] = product(f_s[side], f_s[side]).astype(BF)
        for side in range(2):
            w_s[side] = product(u_s[side], u_s[side]).astype(BF)
        for side in range(2):
            for i in range(0, order, block):
                m_s[side, i : i + block] = product(m_s[side, i : i + block], w_s[side]).astype(BF)
            f_s[side] = factor(side)
        for side in range(2):
            for i in range(0, order, block):
                x_s[side, i : i + block] = product(x_s[side, i : i + block], f_s[side]).astype(BF)
        return carry

    lax.fori_loop(0, ITERS - 1, sweep, 0)
    half = product(x_s[0, pl.ds(pl.multiple_of(off, rows), rows), :], g_s[...]).astype(BF)
    s = product(half, x_s[1])
    return s, jnp.sqrt(jnp.sum(s * s, axis=1, keepdims=True)) + 1e-6


def moments(g, first, second):
    first_new = 0.9 * first + 0.1 * g
    second_new = 0.95 * second + 0.05 * g * g
    step = first_new / (jnp.sqrt(second_new) + 1e-8)
    return first_new, second_new, jnp.sqrt(jnp.sum(step * step, axis=1, keepdims=True))


def root_scratch(order):
    square = lambda dtype: pltpu.VMEM((2, order, order), dtype)
    return [
        pltpu.VMEM((order, order), BF),
        pltpu.VMEM((order, order), BF),
        square(BF),
        square(F32),
    ] + [square(BF)] * 5


def place_of(plan, m, plan_ref, j):
    return lax.rem(plan_ref[plan.row] + m - j, m)


def first_root_kernel(plan, m, plan_ref, *refs):
    grad, stat = refs[:m], refs[m : 2 * m]
    first_ref, second_ref, out_ref = refs[2 * m : 2 * m + 3]
    scratch = refs[2 * m + 3 :]
    g_s, gt_s, stat_s = scratch[:3]
    rows = out_ref.shape[0]
    for j in range(m):
        at = pl.ds(pl.multiple_of(place_of(plan, m, plan_ref, j) * rows, rows), rows)
        g_s[at] = grad[j][...]
        for side in range(2):
            stat_s[side, at] = stat[j][side]
    s, norm = root_rows(plan_ref[plan.row] * rows, rows, g_s, gt_s, stat_s, *scratch[3:])
    adam = moments(grad[0][...].astype(F32), first_ref[0, 0], second_ref[0, 0])[2]
    out_ref[...] = (s * (adam / norm)).astype(BF)


def first_root(plan, m, plan_array, grad, stat, first, second):
    rows, order = grad[0].shape
    slot = pl.BlockSpec((1, 1, rows, order), lambda *_: (0, 0, 0, 0))
    return pl.pallas_call(
        functools.partial(first_root_kernel, plan, m),
        grid=(1,),
        out_shape=shape(rows, order),
        in_specs=[SMEM] + [VMEM] * (2 * m) + [slot, slot],
        out_specs=VMEM,
        scratch_shapes=root_scratch(order),
        compiler_params=params(),
        cost_estimate=cost(20),
    )(plan_array, *grad, *stat, first, second)


def extra_root_kernel(plan, m, plan_ref, *refs):
    own, mate, out_ref, scratch = refs[:m], refs[m : 2 * m], refs[2 * m], refs[2 * m + 1 :]
    g_s, gt_s, stat_s = scratch[:3]
    c = plan_ref[plan.core]
    rows = out_ref.shape[0]
    for j in range(m):
        base = place_of(plan, m, plan_ref, j) * 2
        for source, core in ((own[j], c), (mate[j], 1 - c)):
            at = pl.ds(pl.multiple_of((base + core) * rows, rows), rows)
            g_s[at] = source[0:rows]
            for side in range(2):
                stat_s[side, at] = source[(1 + side) * rows : (2 + side) * rows]
    off = (plan_ref[plan.row] * 2 + c) * rows
    s, norm = root_rows(off, rows, g_s, gt_s, stat_s, *scratch[3:])
    out_ref[...] = (s / norm).astype(BF)


def extra_root(plan, m, plan_array, own, mate):
    rows, order = own[0].shape[0] // 3, own[0].shape[1]
    return pl.pallas_call(
        functools.partial(extra_root_kernel, plan, m),
        out_shape=shape(rows, order),
        in_specs=[SMEM] + [VMEM] * (2 * m),
        out_specs=VMEM,
        scratch_shapes=root_scratch(order),
        compiler_params=params(),
        cost_estimate=cost(20),
    )(plan_array, *own, *mate)


def held_kernel(plan, plan_ref, *refs):
    own, mate = refs[: plan.mid], refs[plan.mid : 2 * plan.mid]
    first_ref, out_ref, flat_own, flat_mate = refs[2 * plan.mid :]
    c = plan_ref[plan.core]
    half_rows = own[0].shape[1]
    for jm in range(plan.mid):
        flat_own[jm * OUTER : (jm + 1) * OUTER] = own[jm][...]
        flat_mate[jm * OUTER : (jm + 1) * OUTER] = mate[jm][...]
    out_ref[0] = first_ref[...]
    for s in range(1, plan.slots):
        at = plan_ref[plan.place + s]
        for source, core in ((flat_own, c), (flat_mate, 1 - c)):
            rows = pl.ds(pl.multiple_of(core * half_rows, half_rows), half_rows)
            out_ref[s, rows] = source[at]


def held_grads(plan, plan_array, own, mate, first_grad):
    rows, columns = first_grad.shape
    flat = pltpu.VMEM((plan.half, rows // 2, columns), BF)
    return pl.pallas_call(
        functools.partial(held_kernel, plan),
        out_shape=shape(plan.slots, rows, columns),
        in_specs=[SMEM] + [VMEM] * (2 * plan.mid + 1),
        out_specs=VMEM,
        scratch_shapes=[flat, flat],
        compiler_params=params(),
        cost_estimate=cost(3),
    )(plan_array, *own, *mate, first_grad)


def moment_kernel(plan, plan_ref, g_ref, first_ref, second_ref, first_out, second_out, norm_out):
    s = pl.program_id(0)
    held = plan_ref[plan.held + s]
    rows = g_ref.shape[1]

    @pl.when(s == 0)
    def _():
        norm_out[...] = jnp.zeros_like(norm_out)

    @pl.when(held == 0)
    def _():
        first_out[...] = first_ref[...]
        second_out[...] = second_ref[...]

    @pl.when(held == 1)
    def _():
        g = g_ref[0].astype(F32)
        first_new, second_new, norm = moments(g, first_ref[0, 0], second_ref[0, 0])
        first_out[0, 0] = first_new
        second_out[0, 0] = second_new

        @pl.when(s > 0)
        def _():
            line = jnp.broadcast_to(norm, (rows, 128)).T
            which = plan_ref[plan.mine + s]
            at = lax.broadcasted_iota(jnp.int32, norm_out.shape, 0) == which
            norm_out[...] = jnp.where(at, line[0:1], norm_out[...])


def moment_update(plan, plan_array, grads, first, second):
    _, slots, rows, columns = first.shape
    slot = pl.BlockSpec((1, 1, rows, columns), lambda s: (0, s, 0, 0))
    return pl.pallas_call(
        functools.partial(moment_kernel, plan),
        grid=(slots,),
        out_shape=(
            shape(*first.shape, dtype=F32),
            shape(*first.shape, dtype=F32),
            shape(plan.half, rows, dtype=F32),
        ),
        in_specs=[SMEM, pl.BlockSpec((1, rows, columns), lambda s: (s, 0, 0)), slot, slot],
        out_specs=(slot, slot, pl.BlockSpec((plan.half, rows), lambda s: (0, 0))),
        compiler_params=params(),
        cost_estimate=cost(6),
    )(plan_array, grads, first, second)


def stat_kernel(plan, m, plan_ref, *refs):
    grad = refs[:m]
    left_ref, right_ref, left_out, right_out, g_s, gt_s = refs[m:]
    s = pl.program_id(0)
    held = plan_ref[plan.held + s]
    rows = grad[0].shape[1]

    @pl.when(held == 0)
    def _():
        left_out[...] = left_ref[...]
        right_out[...] = right_ref[...]

    @pl.when(held == 1)
    def _():
        for j in range(m):
            at = pl.ds(pl.multiple_of(place_of(plan, m, plan_ref, j) * rows, rows), rows)
            g_s[at] = grad[j][0]
        gt_s[...] = transposed(g_s[...])
        mine = pl.ds(pl.multiple_of(plan_ref[plan.row] * rows, rows), rows)
        left_out[0, 0] = 0.9 * left_ref[0, 0] + 0.1 * product(grad[0][0], gt_s[...])
        right_out[0, 0] = 0.9 * right_ref[0, 0] + 0.1 * product(gt_s[mine], g_s[...])


def stat_update(plan, m, plan_array, grads, left, right):
    _, slots, rows, columns = left.shape
    slot = pl.BlockSpec((1, 1, rows, columns), lambda s: (0, s, 0, 0))
    piece = pl.BlockSpec((1, rows, columns), lambda s: (s, 0, 0))
    return pl.pallas_call(
        functools.partial(stat_kernel, plan, m),
        grid=(slots,),
        out_shape=(shape(*left.shape, dtype=F32),) * 2,
        in_specs=[SMEM] + [piece] * m + [slot, slot],
        out_specs=(slot, slot),
        scratch_shapes=[pltpu.VMEM((columns, columns), BF)] * 2,
        compiler_params=params(),
        cost_estimate=cost(10),
    )(plan_array, *grads, left, right)


def final_kernel(plan, plan_ref, *refs):
    mid = plan.mid
    first, extra = refs[: 2 * mid], refs[2 * mid : 4 * mid]
    norm_ref, out_ref, sems = refs[4 * mid :]
    c = plan_ref[plan.core]
    half_rows = extra[0].shape[1]
    copies = []
    for side in range(2):
        for jm in range(mid):
            for jo in range(OUTER):
                j = side * plan.half + jm * OUTER + jo
                copies.append(
                    pltpu.make_async_copy(
                        first[side * mid + jm].at[jo],
                        out_ref.at[plan_ref[plan.final + j]],
                        sems.at[j],
                    )
                )
    for copy in copies:
        copy.start()
    columns = norm_ref[...].T
    lane = lax.broadcasted_iota(jnp.int32, columns.shape, 1)
    for jm in range(mid):
        for jo in range(OUTER):
            j = jm * OUTER + jo
            block = plan_ref[plan.xfinal + j]
            chosen = jnp.where(lane == plan_ref[plan.xindex + j], columns, 0.0)
            norm = jnp.sum(chosen, axis=1, keepdims=True)
            for core in range(2):
                rows = slice(core * half_rows, (core + 1) * half_rows)
                scale = norm[rows]

                @pl.when(c == core)
                def _():
                    out_ref[block, rows] = (extra[jm][jo].astype(F32) * scale).astype(BF)

                @pl.when(c != core)
                def _():
                    out_ref[block, rows] = (extra[mid + jm][jo].astype(F32) * scale).astype(BF)

    for copy in copies:
        copy.wait()


def final_blocks(plan, plan_array, own, mate, extra_own, extra_mate, norms):
    rows, columns = own[0].shape[1:]
    return pl.pallas_call(
        functools.partial(final_kernel, plan),
        out_shape=shape(plan.blocks, rows, columns),
        in_specs=[SMEM] + [ANY] * (2 * plan.mid) + [VMEM] * (2 * plan.mid) + [VMEM],
        out_specs=VMEM,
        scratch_shapes=[pltpu.SemaphoreType.DMA((plan.n,))],
        compiler_params=params(),
        cost_estimate=cost(6),
    )(plan_array, *own, *mate, *extra_own, *extra_mate, norms)


def body(n, m, grads, owners, left, right, first, second):
    slots, blocks, rows = left.shape[1], grads.shape[1], grads.shape[2]
    plan, moves = Plan(n, slots, blocks), Moves(n, m)
    pos = jnp.stack([lax.axis_index("dp"), lax.axis_index("mp")]).astype(jnp.int32)
    plan_array = make_plan(plan, pos, owners[:, 0])
    core = lax.rem(pos[0], 2)

    first_send, extra_send = pick(plan, plan_array, grads)
    stats = jnp.stack([left[0], right[0]])
    mate_rows = lax.dynamic_slice_in_dim(
        stats[:, 1:], (1 - core) * (rows // 2), rows // 2, 2
    ).astype(BF)
    first_got = moves.core(first_send)
    mate_stats = moves.core(mate_rows)
    extra_got = moves.core(extra_send)
    first_stats = moves.rows(stats[:, 0].astype(BF))
    grad0 = scatter(moves, add_first(plan, plan_array, grads, first_got))
    extra = scatter(
        moves, add_extra(plan, plan_array, grads, extra_got, left, right, mate_stats)
    )

    update0 = first_root(plan, m, plan_array, moves.rows(grad0), first_stats, first, second)
    own, mate = gather(moves, update0)

    extra_rows = moves.rows(extra)
    extra_mates = [moves.core(value) for value in extra_rows]
    update_extra = extra_root(plan, m, plan_array, extra_rows, extra_mates)
    extra_own, extra_mate = gather(moves, update_extra)

    grad_own, grad_mate = gather(moves, extra[: rows // 2])
    held = held_grads(plan, plan_array, grad_own, grad_mate, grad0)
    first_out, second_out, norms = moment_update(plan, plan_array, held, first, second)
    norms = norms + moves.core(norms)
    terms = [norms] + [moves.middle(norms, jm) for jm in range(1, moves.mid)]
    norms = sum(terms[1:], terms[0])
    terms = [norms] + [moves.outer(norms, jo) for jo in range(1, OUTER)]
    norms = sum(terms[1:], terms[0])
    left_out, right_out = stat_update(plan, m, plan_array, moves.rows(held), left, right)
    direction = final_blocks(plan, plan_array, own, mate, extra_own, extra_mate, norms)
    return direction, left_out, right_out, first_out, second_out


def solution(mesh):
    n, m = mesh.shape["dp"], mesh.shape["mp"]
    split = P("dp", None, "mp", None)
    return jax.shard_map(
        functools.partial(body, n, m),
        mesh=mesh,
        in_specs=(split, P(), split, split, split, split),
        out_specs=(P(None, "mp", None), split, split, split, split),
        check_vma=False,
    )
```
